32 devices in a mesh: dp: 4 (over x, y), cp: 8 (over z, core).
Axes of the slice: x: 2, y: 2, z: 4, core: 2. Of those that a mesh axis runs over, the one named last changes fastest.
Arguments:
- hidden: bfloat16 [12, 3072, 1792], P('dp', 'cp'), parts along dimension 0
- lengths: int32 [12], P('dp'), parts along dimension 0
- w_qkv: bfloat16 [3, 1792, 5376], replicated
- w_out: bfloat16 [3, 1792, 1792], replicated
- w_in: bfloat16 [3, 1792, 7680], replicated
- w_mlp_out: bfloat16 [3, 3840, 1792], replicated
- attn_gamma: float32 [3, 1792], replicated
- mlp_gamma: float32 [3, 1792], replicated
Outputs:
- output: bfloat16 [12, 3072, 1792], P('dp', 'cp'), parts along dimension 0
There are 4 independent parts. The reference program is written for one: setup_inputs(seed, part) draws one part's arguments, and reference() takes and returns one part's arrays. A program takes and returns all parts, laid end to end along the dimension named above; an argument that names none is the same for every part.
All inputs are finite; a program needn't handle non-finite values.
Results may differ from the reference program's by a relative error of at most 0.0149993.
Values are sent between devices in bfloat16 or wider.
A program may use at most 1 GiB of HBM per device.

```python
import jax
import jax.numpy as jnp
from jax import lax

D_MODEL = 1792
NUM_HEADS = 28
HEAD_DIM = 64
FF_DIM = 3840
DOCS_PART = 3
SEQ_LEN = 3072
WINDOW_HALF = 64
QUERY_BLOCK = 128

THETA_LOCAL = 10000.0
THETA_GLOBAL = 160000.0
LN_EPS = 1e-5
LAYER_GLOBAL = (False, False, True)


def setup_inputs(seed: int = 0, part: int = 0) -> dict:
    part_key = jax.random.fold_in(jax.random.key(seed), part)
    key_noise, key_fast, key_slow, key_len = jax.random.split(part_key, 4)
    fast_len = 32
    slow_count = 8
    fast_count = SEQ_LEN // fast_len
    noise_part = jax.random.normal(key_noise, (DOCS_PART, SEQ_LEN, D_MODEL), jnp.float32)
    fast_topic = jax.random.normal(key_fast, (DOCS_PART, fast_count, 1, D_MODEL), jnp.float32)
    slow_topic = jax.random.normal(key_slow, (DOCS_PART, slow_count, 1, D_MODEL), jnp.float32)
    fast_full = jnp.broadcast_to(fast_topic, (DOCS_PART, fast_count, fast_len, D_MODEL)).reshape(DOCS_PART, SEQ_LEN, D_MODEL)
    slow_full = jnp.broadcast_to(slow_topic, (DOCS_PART, slow_count, SEQ_LEN // slow_count, D_MODEL)).reshape(DOCS_PART, SEQ_LEN, D_MODEL)
    hidden = (0.5 * noise_part + fast_full + slow_full).astype(jnp.bfloat16)
    lengths = jax.random.randint(key_len, (DOCS_PART,), SEQ_LEN // 2, SEQ_LEN + 1, dtype=jnp.int32)
    weight_keys = jax.random.split(jax.random.key(seed + 1), 6)
    w_qkv = jax.random.normal(weight_keys[0], (3, D_MODEL, 3 * D_MODEL), jnp.float32) * D_MODEL ** -0.5
    w_out = jax.random.normal(weight_keys[1], (3, D_MODEL, D_MODEL), jnp.float32) * D_MODEL ** -0.5
    w_in = jax.random.normal(weight_keys[2], (3, D_MODEL, 2 * FF_DIM), jnp.float32) * D_MODEL ** -0.5
    w_mlp_out = jax.random.normal(weight_keys[3], (3, FF_DIM, D_MODEL), jnp.float32) * FF_DIM ** -0.5
    attn_gamma = 1.0 + 0.3 * jax.random.normal(weight_keys[4], (3, D_MODEL), jnp.float32)
    mlp_gamma = 1.0 + 0.3 * jax.random.normal(weight_keys[5], (3, D_MODEL), jnp.float32)
    return {'hidden': hidden, 'lengths': lengths, 'w_qkv': w_qkv.astype(jnp.bfloat16), 'w_out': w_out.astype(jnp.bfloat16), 'w_in': w_in.astype(jnp.bfloat16), 'w_mlp_out': w_mlp_out.astype(jnp.bfloat16), 'attn_gamma': attn_gamma, 'mlp_gamma': mlp_gamma}


def layer_norm(resid, gamma):
    resid_f32 = resid.astype(jnp.float32)
    row_mean = jnp.mean(resid_f32, axis=-1, keepdims=True)
    centered = resid_f32 - row_mean
    row_var = jnp.mean(centered * centered, axis=-1, keepdims=True)
    return (centered * lax.rsqrt(row_var + LN_EPS) * gamma).astype(jnp.bfloat16)


def apply_rope(heads_in, positions, rope_theta):
    half_dim = HEAD_DIM // 2
    inv_freq = rope_theta ** (-jnp.arange(0, HEAD_DIM, 2, dtype=jnp.float32) / HEAD_DIM)
    angles = positions.astype(jnp.float32)[:, None] * inv_freq[None, :]
    cos_tab = jnp.cos(angles)[:, None, :]
    sin_tab = jnp.sin(angles)[:, None, :]
    heads_f32 = heads_in.astype(jnp.float32)
    first_half = heads_f32[..., :half_dim]
    second_half = heads_f32[..., half_dim:]
    return jnp.concatenate([first_half * cos_tab - second_half * sin_tab, second_half * cos_tab + first_half * sin_tab], axis=-1).astype(jnp.bfloat16)


def masked_softmax(scores, allowed):
    scores = jnp.where(allowed, scores, -1e30)
    row_max = jnp.max(scores, axis=-1, keepdims=True)
    exp_scores = jnp.exp(scores - row_max)
    return (exp_scores / jnp.sum(exp_scores, axis=-1, keepdims=True)).astype(jnp.bfloat16)


def finish_rows(attn_out, seq_offset, lengths):
    row_pos = seq_offset + jnp.arange(attn_out.shape[1])
    row_ok = row_pos[None, :, None] < lengths[:, None, None]
    return jnp.where(row_ok, attn_out, 0.0).astype(jnp.bfloat16)


def local_attention(queries, key_val_ext, seq_offset, lengths):
    num_docs, chunk_len, num_heads = queries.shape[:3]
    n_blocks = chunk_len // QUERY_BLOCK
    span_len = 2 * QUERY_BLOCK
    query_blocks = queries.reshape(num_docs, n_blocks, QUERY_BLOCK, num_heads, HEAD_DIM)
    lower_half = key_val_ext[:, :chunk_len].reshape(num_docs, n_blocks, QUERY_BLOCK, 2, num_heads, HEAD_DIM)
    upper_half = key_val_ext[:, QUERY_BLOCK:QUERY_BLOCK + chunk_len].reshape(num_docs, n_blocks, QUERY_BLOCK, 2, num_heads, HEAD_DIM)
    kv_blocks = jnp.concatenate([lower_half, upper_half], axis=2)
    scores = jnp.einsum('bnqhd,bnkhd->bnhqk', query_blocks.astype(jnp.float32), kv_blocks[:, :, :, 0].astype(jnp.float32)) * HEAD_DIM ** -0.5
    row_idx = jnp.arange(QUERY_BLOCK)[:, None]
    col_idx = jnp.arange(span_len)[None, :]
    in_window = (col_idx >= row_idx) & (col_idx <= row_idx + 2 * WINDOW_HALF)
    key_pos = seq_offset - WINDOW_HALF + jnp.arange(n_blocks)[:, None] * QUERY_BLOCK + col_idx
    key_ok = (key_pos >= 0)[None] & (key_pos[None] < lengths[:, None, None])
    allowed = in_window[None, None, None] & key_ok[:, :, None, None, :]
    attn_probs = masked_softmax(scores, allowed)
    attn_out = jnp.einsum('bnhqk,bnkhd->bnqhd', attn_probs.astype(jnp.float32), kv_blocks[:, :, :, 1].astype(jnp.float32))
    return finish_rows(attn_out.reshape(num_docs, chunk_len, num_heads * HEAD_DIM), seq_offset, lengths)


def global_attention(queries, key_val_all, seq_offset, lengths):
    num_docs, chunk_len, num_heads = queries.shape[:3]
    total_len = key_val_all.shape[1]
    n_blocks = chunk_len // QUERY_BLOCK
    query_blocks = jnp.moveaxis(queries.reshape(num_docs, n_blocks, QUERY_BLOCK, num_heads, HEAD_DIM), 1, 0)
    keys_all = key_val_all[:, :, 0].astype(jnp.float32)
    values_all = key_val_all[:, :, 1].astype(jnp.float32)
    key_ok = (jnp.arange(total_len)[None, :] < lengths[:, None])[:, None, None, :]

    def one_block(block_queries):
        scores = jnp.einsum('bqhd,bkhd->bhqk', block_queries.astype(jnp.float32), keys_all) * HEAD_DIM ** -0.5
        attn_probs = masked_softmax(scores, key_ok)
        return jnp.einsum('bhqk,bkhd->bqhd', attn_probs.astype(jnp.float32), values_all)

    block_outs = lax.map(one_block, query_blocks)
    attn_out = jnp.moveaxis(block_outs, 0, 1).reshape(num_docs, chunk_len, num_heads * HEAD_DIM)
    return finish_rows(attn_out, seq_offset, lengths)


def mlp_block(resid, gamma, w_in_layer, w_mlp_out_layer):
    num_docs, seq_count, d_model = resid.shape
    normed = layer_norm(resid, gamma).reshape(num_docs * seq_count, d_model)
    up_proj = jnp.dot(normed, w_in_layer, preferred_element_type=jnp.float32).astype(jnp.bfloat16)
    ff_width = w_mlp_out_layer.shape[0]
    gated_act = (jax.nn.gelu(up_proj[:, :ff_width].astype(jnp.float32), approximate=False) * up_proj[:, ff_width:].astype(jnp.float32)).astype(jnp.bfloat16)
    update = jnp.dot(gated_act, w_mlp_out_layer, preferred_element_type=jnp.float32).reshape(resid.shape)
    return (resid.astype(jnp.float32) + update).astype(jnp.bfloat16)


def reference(hidden, lengths, w_qkv, w_out, w_in, w_mlp_out, attn_gamma, mlp_gamma):
    positions = jnp.arange(SEQ_LEN)
    pad_rows = ((0, 0), (WINDOW_HALF, WINDOW_HALF), (0, 0), (0, 0), (0, 0))

    def one_doc(item):
        doc_hidden, doc_len = item
        resid = doc_hidden[None]
        len_row = doc_len[None]
        for layer_idx in range(3):
            is_global = LAYER_GLOBAL[layer_idx]
            rope_theta = THETA_GLOBAL if is_global else THETA_LOCAL
            normed = layer_norm(resid, attn_gamma[layer_idx]).reshape(SEQ_LEN, D_MODEL)
            qkv_proj = jnp.dot(normed, w_qkv[layer_idx], preferred_element_type=jnp.float32).astype(jnp.bfloat16).reshape(1, SEQ_LEN, 3, NUM_HEADS, HEAD_DIM)
            queries = apply_rope(qkv_proj[:, :, 0], positions, rope_theta)
            keys_rot = apply_rope(qkv_proj[:, :, 1], positions, rope_theta)
            key_val = jnp.stack([keys_rot, qkv_proj[:, :, 2]], axis=2)
            if is_global:
                attn_out = global_attention(queries, key_val, 0, len_row)
            else:
                attn_out = local_attention(queries, jnp.pad(key_val, pad_rows), 0, len_row)
            proj_out = jnp.dot(attn_out.reshape(SEQ_LEN, D_MODEL), w_out[layer_idx], preferred_element_type=jnp.float32)
            resid = (resid.astype(jnp.float32) + proj_out.reshape(resid.shape)).astype(jnp.bfloat16)
            resid = mlp_block(resid, mlp_gamma[layer_idx], w_in[layer_idx], w_mlp_out[layer_idx])
        return resid[0]

    return lax.map(one_doc, (hidden, lengths))
```

```python
import functools

import jax
import jax.numpy as jnp
from jax import lax
from jax.experimental import pallas as pl
from jax.experimental.pallas import tpu as pltpu
from jax.sharding import PartitionSpec as P


D = 1792
FF = 3840
HEAD_DIM = 64
HALO = 64
ROWS = 384
SEQ = 3072
GROUP = 8
OWNERS = 7
WIDE = 256
N_HEADS_WIDE = D // WIDE
T_OUT = 896
N_OUT = D // T_OUT
TILE = 768
N_QKV = 3 * D // TILE
N_MLP = FF // TILE
GQ = 1024
GK = 1024
VMEM_LIMIT = 66 * 1000 * 1000
THETA_LOCAL = 10000.0
THETA_GLOBAL = 160000.0
LN_EPS = 1e-5
NEG = -1e30
F32 = jnp.float32
BF16 = jnp.bfloat16


def dot(a, b):
    return lax.dot_general(a, b, (((1,), (0,)), ((), ())), preferred_element_type=F32)


def rope_tables(positions, theta):
    inv_freq = theta ** (-jnp.arange(0, HEAD_DIM, 2, dtype=F32) / HEAD_DIM)
    angles = positions.astype(F32)[:, None] * inv_freq[None, :]
    cos, sin = jnp.cos(angles), jnp.sin(angles)
    return jnp.concatenate([cos] * 4, axis=1), jnp.concatenate([-sin, sin, -sin, sin], axis=1)


def rotate(y, cos, sin):
    y = y.astype(BF16).astype(F32)
    lane = lax.broadcasted_iota(jnp.int32, (1, 128), 1)
    low = lane % HEAD_DIM < HEAD_DIM // 2
    parts = []
    for c in range(y.shape[1] // 128):
        part = y[:, c * 128:(c + 1) * 128]
        other = jnp.where(low, pltpu.roll(part, 96, 1), pltpu.roll(part, 32, 1))
        parts.append(part * cos + other * sin)
    return jnp.concatenate(parts, axis=1).astype(BF16)


def norm_rows(src, gamma, dst, n_rows, step=16):
    def one(r, carry):
        rows = pl.ds(pl.multiple_of(r * step, step), step)
        x = src[rows, :].astype(BF16).astype(F32)
        mean = jnp.sum(x, axis=1, keepdims=True) * (1.0 / D)
        c = x - mean
        var = jnp.sum(c * c, axis=1, keepdims=True) * (1.0 / D)
        dst[rows, :] = (c * lax.rsqrt(var + LN_EPS) * gamma).astype(BF16)
        return carry

    lax.fori_loop(0, n_rows // step, one, 0, unroll=2)


def gelu_gate(u):
    a = u[:, :TILE].astype(F32)
    g = u[:, TILE:].astype(F32)
    return (a * (0.5 * (1.0 + lax.erf(a * (2.0 ** -0.5)))) * g).astype(BF16)


def rope_pass(out, groups, cos, sin, step=32):
    def one(r, carry):
        src = pl.ds(pl.multiple_of(r * step, step), step)
        c, s = cos[src, :], sin[src, :]
        for doc in range(out.shape[0] // ROWS):
            rows = pl.ds(pl.multiple_of(doc * ROWS + r * step, step), step)
            for g in range(groups):
                cols = slice(g * 128, (g + 1) * 128)
                out[rows, cols] = rotate(out[rows, cols], c, s)
        return carry

    lax.fori_loop(0, ROWS // step, one, 0)


def qkv_tile(t, h, w_qkv, cos, sin, qkv):
    qkv[...] = dot(h[...], w_qkv).astype(BF16)
    whole_tiles, rest = divmod(2 * D, TILE)

    @pl.when(t < whole_tiles)
    def _():
        rope_pass(qkv, TILE // 128, cos, sin)

    @pl.when(t == whole_tiles)
    def _():
        rope_pass(qkv, rest // 128, cos, sin)


def first_kernel(layer, after, x, w_qkv, gamma, cos, sin, qkv, h):
    t = pl.program_id(0)

    @pl.when(t == 0)
    def _():
        norm_rows(x, gamma[layer:layer + 1, :], h, x.shape[0])

    qkv_tile(t, h, w_qkv[...], cos, sin, qkv)


def whole(shape):
    return pl.BlockSpec(shape, lambda *_: (0,) * len(shape), pipeline_mode=pl.Buffered(1))


def cost(flops, nbytes):
    return pl.CostEstimate(flops=int(flops * 0.01), bytes_accessed=int(nbytes), transcendentals=0)


def first_block(after, x, w_qkv, gamma, cos, sin, layer):
    n_rows = x.shape[0]
    return pl.pallas_call(
        functools.partial(first_kernel, layer),
        grid=(N_QKV,),
        in_specs=[pl.BlockSpec(memory_space=pl.ANY), whole((n_rows, D)), pl.BlockSpec((None, D, TILE), lambda i: (layer, 0, i)), whole((3, D)), whole((ROWS, 128)), whole((ROWS, 128))],
        out_specs=pl.BlockSpec((n_rows, TILE), lambda i: (0, i)),
        out_shape=jax.ShapeDtypeStruct((n_rows, 3 * D), BF16),
        scratch_shapes=[pltpu.VMEM((n_rows, D), BF16)],
        cost_estimate=cost(2 * n_rows * D * 3 * D, 2 * D * 3 * D),
        compiler_params=pltpu.CompilerParams(vmem_limit_bytes=VMEM_LIMIT),
        name="first_qkv",
    )(after, x, w_qkv, gamma, cos, sin)


def post_kernel(layer, mode, n_o, *refs):
    refs = list(refs)
    where, _ = refs.pop(0), refs.pop(0)
    o_refs = [refs.pop(0) for _ in range(n_o)]
    x, w_out, w_in, w_mlp_out, mlp_gamma = [refs.pop(0) for _ in range(5)]
    if mode == "qkv":
        w_qkv, attn_gamma, cos, sin = [refs.pop(0) for _ in range(4)]
        x_out, qkv = refs.pop(0), refs.pop(0)
    elif mode == "norm":
        attn_gamma = refs.pop(0)
        x_out, h_out = refs.pop(0), refs.pop(0)
    else:
        x_out = refs.pop(0)
    h, acc, u_even, u_odd, wo, wa, wg, wd, sem_o, sem_a, sem_g, sem_d = [refs.pop(0) for _ in range(12)]
    if mode == "qkv":
        wq, sem_q = refs.pop(0), refs.pop(0)
    o_full = refs.pop(0) if n_o > 1 else o_refs[0]
    n_rows = x.shape[0]
    i = pl.program_id(0)
    j = i - N_OUT

    def tile(t):
        return pl.ds(pl.multiple_of(t * TILE, 128), TILE)

    def out_copy(c):
        cols = pl.ds(pl.multiple_of(c * T_OUT, 128), T_OUT)
        return pltpu.make_async_copy(w_out.at[layer, :, cols], wo.at[c], sem_o.at[c])

    def up_copies(t):
        slot = lax.rem(t, 2)
        gate = pl.ds(pl.multiple_of(FF + t * TILE, 128), TILE)
        return (
            pltpu.make_async_copy(w_in.at[layer, :, tile(t)], wa.at[slot], sem_a.at[slot]),
            pltpu.make_async_copy(w_in.at[layer, :, gate], wg.at[slot], sem_g.at[slot]),
        )

    def down_copy(t):
        slot = lax.rem(t, 2)
        return pltpu.make_async_copy(w_mlp_out.at[layer, tile(t), :], wd.at[slot], sem_d.at[slot])

    def qkv_copy(t):
        slot = lax.rem(t, 2)
        return pltpu.make_async_copy(w_qkv.at[layer + 1, :, tile(t)], wq.at[slot], sem_q.at[slot])

    @pl.when(i == 0)
    def _():
        for c in range(N_OUT):
            out_copy(jnp.int32(c)).start()
        for c in up_copies(jnp.int32(0)):
            c.start()
        down_copy(jnp.int32(0)).start()
        if n_o > 1:
            for k in range(n_o):
                source = lax.rem(where[0] - k + n_o, n_o)

                @pl.when(source < OWNERS)
                def _():
                    o_full[:, pl.ds(pl.multiple_of(source * WIDE, WIDE), WIDE)] = o_refs[k][...]

    @pl.when(i < N_OUT)
    def _():
        out_copy(i).wait()
        cols = pl.ds(pl.multiple_of(i * T_OUT, 128), T_OUT)
        acc[:, cols] = (x[:, cols].astype(F32) + dot(o_full[...], wo[i])).astype(BF16).astype(F32)

    @pl.when(j == 0)
    def _():
        norm_rows(acc, mlp_gamma[layer:layer + 1, :], h, n_rows)

    @pl.when((j >= 0) & (j < N_MLP - 1))
    def _():
        for c in up_copies(j + 1):
            c.start()

    @pl.when((j >= 1) & (j < N_MLP))
    def _():
        down_copy(j).start()

    @pl.when((j >= 0) & (j < N_MLP))
    def _():
        for c in up_copies(j):
            c.wait()

    @pl.when((j >= 1) & (j <= N_MLP))
    def _():
        down_copy(j - 1).wait()

    if mode == "qkv":
        @pl.when((j >= N_MLP - 1) & (j <= N_MLP))
        def _():
            qkv_copy(j - N_MLP + 1).start()

    slot = lax.rem(jnp.maximum(j, 0), 2)

    def project(u):
        u[:, :TILE] = dot(h[...], wa[slot]).astype(BF16)
        u[:, TILE:] = dot(h[...], wg[slot]).astype(BF16)

    def consume(u):
        acc[...] += dot(gelu_gate(u[...]), wd[1 - slot])

    @pl.when(j == 0)
    def _():
        project(u_even)

    @pl.when((j > 0) & (j < N_MLP) & (slot == 1))
    def _():
        consume(u_even)
        project(u_odd)

    @pl.when((j > 0) & (j < N_MLP) & (slot == 0))
    def _():
        consume(u_odd)
        project(u_even)

    @pl.when(j == N_MLP)
    def _():
        consume(u_even if (N_MLP - 1) % 2 == 0 else u_odd)
        x_out[...] = acc[...].astype(BF16)
        if mode == "qkv":
            norm_rows(acc, attn_gamma[layer + 1:layer + 2, :], h, n_rows)
        elif mode == "norm":
            norm_rows(acc, attn_gamma[layer + 1:layer + 2, :], h_out, n_rows)

    if mode == "qkv":
        t = j - N_MLP - 1

        @pl.when(t >= 0)
        def _():
            qkv_copy(t).wait()
            qkv_tile(t, h, wq[lax.rem(t, 2)], cos, sin, qkv)

        @pl.when((t >= 0) & (t < N_QKV - 2))
        def _():
            qkv_copy(t + 2).start()


def post_block(after, where, o_parts, x, weights, layer, mode, cos=None, sin=None):
    w_qkv, w_out, w_in, w_mlp_out, attn_gamma, mlp_gamma = weights
    n_o = len(o_parts)
    n_rows = x.shape[0]
    base = N_OUT + N_MLP + 1
    steps = base + (N_QKV if mode == "qkv" else 0)
    hbm = pl.BlockSpec(memory_space=pl.ANY)
    full = whole((n_rows, D))
    in_specs = [hbm] + [whole(o.shape) for o in o_parts] + [full, hbm, hbm, hbm, whole((3, D))]
    args = [after] + list(o_parts) + [x, w_out, w_in, w_mlp_out, mlp_gamma]
    out_specs = [full]
    out_shape = [jax.ShapeDtypeStruct((n_rows, D), BF16)]
    flops = 2 * n_rows * D * (D + 3 * FF)
    sem = pltpu.SemaphoreType.DMA((2,))
    scratch = [
        pltpu.VMEM((n_rows, D), BF16),
        pltpu.VMEM((n_rows, D), F32),
        pltpu.VMEM((n_rows, 2 * TILE), BF16),
        pltpu.VMEM((n_rows, 2 * TILE), BF16),
        pltpu.VMEM((2, D, T_OUT), BF16),
        pltpu.VMEM((2, D, TILE), BF16),
        pltpu.VMEM((2, D, TILE), BF16),
        pltpu.VMEM((2, TILE, D), BF16),
        sem, sem, sem, sem,
    ]
    if mode == "qkv":
        in_specs += [hbm, whole((3, D)), whole((ROWS, 128)), whole((ROWS, 128))]
        args += [w_qkv, attn_gamma, cos, sin]
        out_specs.append(pl.BlockSpec((n_rows, TILE), lambda i, *_: (0, jnp.clip(i - base, 0, N_QKV - 1))))
        out_shape.append(jax.ShapeDtypeStruct((n_rows, 3 * D), BF16))
        flops += 2 * n_rows * D * 3 * D
        scratch += [pltpu.VMEM((2, D, TILE), BF16), sem]
    elif mode == "norm":
        in_specs.append(whole((3, D)))
        args.append(attn_gamma)
        out_specs.append(full)
        out_shape.append(jax.ShapeDtypeStruct((n_rows, D), BF16))
    if n_o > 1:
        scratch.append(pltpu.VMEM((n_rows, D), BF16))
    return pl.pallas_call(
        functools.partial(post_kernel, layer, mode, n_o),
        grid_spec=pltpu.PrefetchScalarGridSpec(
            num_scalar_prefetch=1, grid=(steps,), in_specs=in_specs, out_specs=out_specs, scratch_shapes=scratch
        ),
        out_shape=out_shape,
        cost_estimate=cost(flops, flops / n_rows),
        compiler_params=pltpu.CompilerParams(vmem_limit_bytes=VMEM_LIMIT),
    )(where, *args)


def local_kernel(where, after, q, k, v, pk, pv, nk, nv, out, bias):
    offset, length = where[0], where[1 + pl.program_id(0)]

    @pl.when(pl.program_id(1) == 0)
    def _():
        row = lax.broadcasted_iota(jnp.int32, (256, 256), 0) % 128
        col = lax.broadcasted_iota(jnp.int32, (256, 256), 1)
        window = (col >= row) & (col <= row + 2 * HALO)
        for b in range(ROWS // 128):
            pos = offset - HALO + b * 128 + col
            bias[b] = jnp.where(window & (pos >= 0) & (pos < length), 0.0, NEG)

    low = lax.broadcasted_iota(jnp.int32, (1, 128), 1) < HEAD_DIM
    for pair in range(WIDE // 128):
        cols = slice(pair * 128, (pair + 1) * 128)
        k_t = jnp.concatenate([pk[:, cols], k[:, cols], nk[:, cols]], axis=0).T
        v_ext = jnp.concatenate([pv[:, cols], v[:, cols], nv[:, cols]], axis=0)
        n_blocks = ROWS // 128
        rows = [slice(b * 128, (b + 1) * 128) for b in range(n_blocks)]
        spans = [slice(b * 128, b * 128 + 256) for b in range(n_blocks)]
        scores = []
        for b in range(n_blocks):
            qs = q[rows[b], cols] * jnp.asarray(HEAD_DIM ** -0.5, BF16)
            zero = jnp.zeros_like(qs)
            both = jnp.concatenate([jnp.where(low, qs, zero), jnp.where(low, zero, qs)], axis=0)
            scores.append(dot(both, k_t[:, spans[b]]) + bias[b])
        exps = [jnp.exp(s - jnp.max(s, axis=1, keepdims=True)) for s in scores]
        sums = [jnp.sum(e, axis=1, keepdims=True) for e in exps]
        for b in range(n_blocks):
            o = dot(exps[b].astype(BF16), v_ext[spans[b]]) * (1.0 / sums[b])
            ok = offset + b * 128 + lax.broadcasted_iota(jnp.int32, (128, 1), 0) < length
            out[rows[b], cols] = jnp.where(ok, jnp.where(low, o[:128], o[128:]), 0.0).astype(BF16)


def local_block(after, where, qkv, prev, nxt):
    n_rows = qkv.shape[0]

    def main(part):
        return pl.BlockSpec((ROWS, WIDE), lambda d, i, *_: (d, part * N_HEADS_WIDE + i))

    def edge(part):
        return pl.BlockSpec((HALO, WIDE), lambda d, i, *_: (d, part * N_HEADS_WIDE + i))

    return pl.pallas_call(
        local_kernel,
        grid_spec=pltpu.PrefetchScalarGridSpec(
            num_scalar_prefetch=1,
            grid=(n_rows // ROWS, N_HEADS_WIDE),
            in_specs=[pl.BlockSpec(memory_space=pl.ANY), main(0), main(1), main(2), edge(0), edge(1), edge(0), edge(1)],
            out_specs=main(0),
            scratch_shapes=[pltpu.VMEM((ROWS // 128, 256, 256), F32)],
        ),
        out_shape=jax.ShapeDtypeStruct((n_rows, D), BF16),
        cost_estimate=cost(15e6 * n_rows, 6 * n_rows * D),
        name="local_attn",
    )(where, after, qkv, qkv, qkv, prev, prev, nxt, nxt)


def project_kernel(where, after, h, wq, wk, wv, cos, sin, q, k_t, v):
    @pl.when(pl.program_id(0) * 512 < where[1])
    def _():
        hv = h[...]
        q[...] = rotate(dot(hv, wq[...]), cos[...], sin[...]) * jnp.asarray(HEAD_DIM ** -0.5, BF16)
        k_t[...] = rotate(dot(hv, wk[...]), cos[...], sin[...]).T
        v[...] = dot(hv, wv[...]).astype(BF16)

    @pl.when(pl.program_id(0) * 512 >= where[1])
    def _():
        for ref in (q, k_t, v):
            ref[...] = jnp.zeros_like(ref)


def project_block(after, where, h_all, w_qkv, cos, sin):
    def weight(part):
        return pl.BlockSpec((None, D, WIDE), lambda i, where: (2, 0, part * N_HEADS_WIDE + where[0]))

    rows = pl.BlockSpec((512, WIDE), lambda i, *_: (i, 0))
    table = pl.BlockSpec((512, 128), lambda i, *_: (i, 0))
    shape = jax.ShapeDtypeStruct((SEQ, WIDE), BF16)
    return pl.pallas_call(
        project_kernel,
        grid_spec=pltpu.PrefetchScalarGridSpec(
            num_scalar_prefetch=1,
            grid=(SEQ // 512,),
            in_specs=[pl.BlockSpec(memory_space=pl.ANY), pl.BlockSpec((512, D), lambda i, *_: (i, 0)), weight(0), weight(1), weight(2), table, table],
            out_specs=[rows, pl.BlockSpec((WIDE, 512), lambda i, *_: (0, i)), rows],
        ),
        out_shape=[shape, jax.ShapeDtypeStruct((WIDE, SEQ), BF16), shape],
        cost_estimate=cost(2 * SEQ * D * 3 * WIDE, 2 * SEQ * D),
        name="global_qkv",
    )(where, after, h_all, w_qkv, w_qkv, w_qkv, cos, sin)


def global_kernel(where, q, k_t, v, out, s_even, s_odd, m_ref, l_ref, acc_ref):
    length = where[1]
    start = pl.program_id(0) * GQ
    low = lax.broadcasted_iota(jnp.int32, (1, 128), 1) < HEAD_DIM
    scores = (s_even, s_odd)

    def head_step(following, current, top):
        if following is not None:
            cols = slice((following // 2) * 128, (following // 2) * 128 + 128)
            qp = q[:, cols]
            qn = jnp.where(low == (following % 2 == 0), qp, jnp.zeros_like(qp))
            m_ref[...] = jnp.full_like(m_ref, -jnp.inf)
        if current is not None:
            v_cols = slice((current // 2) * 128, (current // 2) * 128 + 128)
            l_ref[...] = jnp.zeros_like(l_ref)
            acc_ref[current % 2] = jnp.zeros((GQ, 128), F32)

        def chunk(c, masked):
            keys = pl.ds(pl.multiple_of(c * GK, GK), GK)
            if following is not None:
                s = dot(qn, k_t[cols, keys])
                if masked:
                    pos = c * GK + lax.broadcasted_iota(jnp.int32, (1, GK), 1)
                    s = s + jnp.where(pos < length, 0.0, NEG)
                scores[following % 2][:, keys] = s
                best = s[:, :128]
                for g in range(1, GK // 128):
                    best = jnp.maximum(best, s[:, g * 128:(g + 1) * 128])
                m_ref[...] = jnp.maximum(m_ref[...], best)
            if current is not None:
                e = jnp.exp(scores[current % 2][:, keys] - top)
                part = e[:, :128]
                for g in range(1, GK // 128):
                    part = part + e[:, g * 128:(g + 1) * 128]
                l_ref[...] += part
                acc_ref[current % 2] += dot(e.astype(BF16), v[keys, v_cols])

        def full_chunk(c, carry):
            chunk(c, False)
            return carry

        n_full = length // GK
        lax.fori_loop(0, n_full, full_chunk, 0)

        @pl.when(n_full * GK < length)
        def _():
            chunk(n_full, True)

        if current is not None:
            acc_ref[current % 2] *= 1.0 / jnp.sum(l_ref[...], axis=1, keepdims=True)
        return None if following is None else jnp.max(m_ref[...], axis=1, keepdims=True)

    @pl.when(start >= length)
    def _():
        out[...] = jnp.zeros_like(out)

    @pl.when(start < length)
    def _():
        ok = start + lax.broadcasted_iota(jnp.int32, (GQ, 1), 0) < length
        top = head_step(0, None, None)
        for head in range(4):
            top = head_step(head + 1 if head < 3 else None, head, top)
            if head % 2 == 1:
                o = jnp.where(low, acc_ref[0], acc_ref[1])
                out[:, (head // 2) * 128:(head // 2) * 128 + 128] = jnp.where(ok, o, 0.0).astype(BF16)


def global_block(where, q, k_t, v):
    rows = pl.BlockSpec((GQ, WIDE), lambda i, *_: (i, 0))
    return pl.pallas_call(
        global_kernel,
        grid_spec=pltpu.PrefetchScalarGridSpec(
            num_scalar_prefetch=1,
            grid=(SEQ // GQ,),
            in_specs=[rows, whole((WIDE, SEQ)), whole((SEQ, WIDE))],
            out_specs=rows,
            scratch_shapes=[pltpu.VMEM((GQ, SEQ), F32)] * 2 + [pltpu.VMEM((GQ, 128), F32)] * 2 + [pltpu.VMEM((2, GQ, 128), F32)],
        ),
        out_shape=jax.ShapeDtypeStruct((SEQ, WIDE), BF16),
        cost_estimate=cost(50e9, 8 * SEQ * WIDE),
        compiler_params=pltpu.CompilerParams(vmem_limit_bytes=VMEM_LIMIT),
        name="global_attn",
    )(where, q, k_t, v)


def solution(mesh):
    to_next = [(d, d + 1) for d in range(GROUP - 1)]
    to_prev = [(d + 1, d) for d in range(GROUP - 1)]

    def layers(hidden, lengths, w_qkv, w_out, w_in, w_mlp_out, attn_gamma, mlp_gamma):
        weights = (w_qkv, w_out, w_in, w_mlp_out, attn_gamma, mlp_gamma)
        me = lax.axis_index('cp').astype(jnp.int32)
        offset = me * ROWS
        cos_l, sin_l = rope_tables(offset + jnp.arange(ROWS), THETA_LOCAL)
        cos_g, sin_g = rope_tables(jnp.arange(SEQ), THETA_GLOBAL)
        at = me[None]
        n_docs = hidden.shape[0]

        docs = range(n_docs)
        xs = [hidden[doc] for doc in docs]
        wheres = [jnp.stack([offset, lengths[doc]]) for doc in docs]
        qkvs, edges, gathered = [None] * n_docs, [None] * n_docs, [None] * n_docs
        last = lengths

        def exchange(doc, qkv):
            qkvs[doc] = qkv
            prev = lax.ppermute(qkv[ROWS - HALO:, D:], 'cp', to_next)
            edges[doc] = prev, lax.ppermute(qkv[:HALO, D:], 'cp', to_prev)

        for doc in docs:
            last = first_block(last, xs[doc], w_qkv, attn_gamma, cos_l, sin_l, 0)
            exchange(doc, last)
        for layer, doc in ((0, 0), (0, 1), (1, 0), (0, 2), (1, 1), (1, 2)):
            o = local_block(last, wheres[doc], qkvs[doc], *edges[doc])
            if layer == 0:
                xs[doc], last = post_block(o, at, [o], xs[doc], weights, 0, "qkv", cos_l, sin_l)
                exchange(doc, last)
            else:
                xs[doc], last = post_block(o, at, [o], xs[doc], weights, 1, "norm")
                gathered[doc] = lax.all_gather(last, 'cp', axis=0, tiled=True)

        attended = []
        for doc in docs:
            where = jnp.stack([jnp.minimum(me, OWNERS - 1), lengths[doc]])
            q, k_t, v = project_block(last, where, gathered[doc], w_qkv, cos_g, sin_g)
            last = global_block(where, q, k_t, v)
            attended.append(last.reshape(GROUP, ROWS, WIDE))

        outs = []
        for lo, hi in ((0, n_docs - 1), (n_docs - 1, n_docs)):
            parts = []
            for k_off in range(GROUP):
                target = lax.rem(me + k_off, GROUP)
                piece = jnp.concatenate([lax.dynamic_index_in_dim(o, target, 0, keepdims=False) for o in attended[lo:hi]], axis=0)
                pairs = [(d, (d + k_off) % GROUP) for d in range(OWNERS)]
                parts.append(lax.ppermute(piece, 'cp', pairs) if k_off else piece)
            x, = post_block(last, at, parts, jnp.concatenate(xs[lo:hi], axis=0), weights, 2, "last")
            outs.append(x)
            last = x
        return jnp.concatenate(outs, axis=0).reshape(n_docs, ROWS, D)

    act_spec = P('dp', 'cp', None)
    return jax.shard_map(layers, mesh=mesh, in_specs=(act_spec, P('dp'), P(), P(), P(), P(), P(), P()), out_specs=act_spec, check_vma=False)
```
